16 devices in a mesh: rep: 2 (over y, z), dp: 8 (over x, core).
Axes of the slice: x: 4, y: 2, z: 1, core: 2. Of those that a mesh axis runs over, the one named last changes fastest.
The devices are a block of a 4x4x8 slice.
Arguments:
- x: bfloat16 [16, 2048, 1024], P(('rep', 'dp')), parts along dimension 0
- dy: bfloat16 [16, 2048, 1024], P(('rep', 'dp')), parts along dimension 0
- w_gate: bfloat16 [2, 1024, 3200], replicated
- w_up: bfloat16 [2, 1024, 3200], replicated
- w_down: bfloat16 [2, 3200, 1024], replicated
- m_w_gate: float32 [2, 1024, 3200], P(None, 'dp')
- m_w_up: float32 [2, 1024, 3200], P(None, 'dp')
- m_w_down: float32 [2, 3200, 1024], P(None, 'dp')
- v_w_gate: float32 [2, 1024, 3200], P(None, 'dp')
- v_w_up: float32 [2, 1024, 3200], P(None, 'dp')
- v_w_down: float32 [2, 3200, 1024], P(None, 'dp')
Outputs:
- output 1: bfloat16 [4, 1024, 3200], P('rep'), parts along dimension 0
- output 2: bfloat16 [4, 1024, 3200], P('rep'), parts along dimension 0
- output 3: bfloat16 [4, 3200, 1024], P('rep'), parts along dimension 0
- output 4: float32 [4, 1024, 3200], P('rep', 'dp'), parts along dimension 0
- output 5: float32 [4, 1024, 3200], P('rep', 'dp'), parts along dimension 0
- output 6: float32 [4, 3200, 1024], P('rep', 'dp'), parts along dimension 0
- output 7: float32 [4, 1024, 3200], P('rep', 'dp'), parts along dimension 0
- output 8: float32 [4, 1024, 3200], P('rep', 'dp'), parts along dimension 0
- output 9: float32 [4, 3200, 1024], P('rep', 'dp'), parts along dimension 0
There are 2 independent parts. The reference program is written for one: setup_inputs(seed, part) draws one part's arguments, and reference() takes and returns one part's arrays. A program takes and returns all parts, laid end to end along the dimension named above; an argument that names none is the same for every part.
All inputs are finite; a program needn't handle non-finite values.
Results may differ from the reference program's by a relative error of at most 0.022.
Values are sent between devices in bfloat16 or wider.
A program may use at most 768 MiB of HBM per device.

```python
import jax
import jax.numpy as jnp
from jax import lax

SEQUENCES = 8
TOKENS = 2048
D = 1024
FF = 3200
LAYERS = 2
NAMES = ("w_gate", "w_up", "w_down")
SHAPES = {"w_gate": (LAYERS, D, FF), "w_up": (LAYERS, D, FF), "w_down": (LAYERS, FF, D)}


def bump(key, n, height):
    away = (jnp.arange(n, dtype=jnp.int32) - jax.random.randint(key, (), 0, n, jnp.int32)) % n
    return jnp.where(away < n // 8, height, 1.0)


def together(key, own, strength):
    shared = jax.random.normal(key, own.shape[1:], jnp.float32)
    return (own + strength * shared) * lax.rsqrt(1 + strength * strength)


def setup_inputs(seed: int = 0, part: int = 0) -> dict:
    kx, kdy, ka, kb, kz, kf, kh, kl, *keys = jax.random.split(jax.random.key(seed), 8 + 3 * len(NAMES))
    kx, kdy, ka, kb = (jax.random.fold_in(k, part) for k in (kx, kdy, ka, kb))
    kw, km, kv = (keys[i::3] for i in range(3))
    shape = (SEQUENCES, TOKENS, D)
    much_x, much_dy = jax.random.uniform(kz, (2,), jnp.float32, 0.0, 1.0)
    loud = 2.0 ** jax.random.uniform(jax.random.fold_in(kz, 1), (), jnp.float32, -1.0, 2.0)
    layers = 2.0 ** jax.random.uniform(kl, (LAYERS, 1, 1), jnp.float32, -1.0, 1.0)
    x = together(ka, jax.random.normal(kx, shape, jnp.float32), much_x) * bump(kf, D, 4.0)
    dy = together(kb, jax.random.normal(kdy, shape, jnp.float32), much_dy)
    drawn = {"x": x.astype(jnp.bfloat16), "dy": (loud * dy * (SEQUENCES * TOKENS) ** -0.5).astype(jnp.bfloat16)}
    for key, name in zip(kw, NAMES, strict=True):
        w = jax.random.normal(key, SHAPES[name], jnp.float32) * SHAPES[name][1] ** -0.5
        drawn[name] = (w * {"w_gate": 1.0, "w_up": bump(kh, FF, 4.0), "w_down": layers}[name]).astype(jnp.bfloat16)
    for key, name in zip(km, NAMES, strict=True):
        drawn[f"m_{name}"] = 0.1 * jax.random.normal(key, SHAPES[name], jnp.float32)
    for key, name in zip(kv, NAMES, strict=True):
        drawn[f"v_{name}"] = jax.random.uniform(key, SHAPES[name], jnp.float32, 0.005, 0.015)
    return drawn


def matmul(a, w):
    return jnp.dot(a, w, preferred_element_type=jnp.float32).astype(jnp.bfloat16)


def normed(h):
    wide = h.astype(jnp.float32)
    scale = lax.rsqrt(jnp.mean(wide**2, -1, keepdims=True) + 1e-6)
    return (wide * scale).astype(jnp.bfloat16)


def layer(h, w):
    a = normed(h)
    gate = jnp.dot(a, w["w_gate"], preferred_element_type=jnp.float32)
    up = jnp.dot(a, w["w_up"], preferred_element_type=jnp.float32)
    return h + matmul((jax.nn.silu(gate) * up).astype(jnp.bfloat16), w["w_down"])


def adamw(w, m, v, g):
    m = 0.9 * m + 0.1 * g
    v = 0.95 * v + 0.05 * g * g
    step = m * lax.rsqrt(v + 1e-8) + 0.1 * w
    return (w - 0.02 * step).astype(jnp.bfloat16), m, v


def stack(weights, h):
    return lax.scan(lambda h, w: (layer(h, w), None), h, weights)[0]


def reference(x, dy, w_gate, w_up, w_down, m_w_gate, m_w_up, m_w_down, v_w_gate, v_w_up, v_w_down):
    weights = dict(zip(NAMES, (w_gate, w_up, w_down), strict=True))

    def take(so_far, sequence):
        h, by_y = sequence
        _, back = jax.vjp(lambda w: stack(w, h), weights)
        return jax.tree.map(lambda total, term: total + term.astype(jnp.float32), so_far, back(by_y)[0]), None

    none_yet = {name: jnp.zeros(w.shape, jnp.float32) for name, w in weights.items()}
    by_weights, _ = lax.scan(take, none_yet, (x, dy))
    gradients = [by_weights[name].astype(jnp.bfloat16).astype(jnp.float32) for name in NAMES]
    new = [
        adamw(w.astype(jnp.float32), m, v, g)
        for w, m, v, g in zip((w_gate, w_up, w_down), (m_w_gate, m_w_up, m_w_down), (v_w_gate, v_w_up, v_w_down), gradients, strict=True)
    ]
    return tuple(one[which] for which in range(3) for one in new)
```

```python
import functools

import jax
import jax.numpy as jnp
from jax import lax
from jax.experimental import pallas as pl
from jax.experimental.pallas import tpu as pltpu
from jax.sharding import PartitionSpec as P

F32, BF16 = jnp.float32, jnp.bfloat16
PIECES = 5
TILE = 512
MESH = pl.DeviceIdType.MESH


def dot(a, b, ca=1, cb=0):
    return lax.dot_general(a, b, (((ca,), (cb,)), ((), ())), preferred_element_type=F32)


def norm(h):
    wide = h.astype(F32)
    scale = lax.rsqrt(jnp.mean(wide * wide, -1, keepdims=True) + 1e-6)
    return (wide * scale).astype(BF16)


def new_moments(m, v, g):
    return 0.9 * m + 0.1 * g, 0.95 * v + 0.05 * g * g


class Kind:
    pass


def wide_sum(*parts):
    total = parts[0].astype(F32)
    for part in parts[1:]:
        total = total + part.astype(F32)
    return total


def kernel(dims, *refs):
    T, D, FF, C, R, RB, PB = dims
    it = iter(refs)
    take = lambda n: [next(it) for _ in range(n)]
    a1, a1t, dy, dyt, h1, a0, a0t = take(7)
    wg, wu, wd, mg, mu, md, vg, vu, vd = take(9)
    nw_a, nw_b, g_a, g_b, dwd = take(5)
    a, at, d, dt, da, wgc, wuc, wdc, act, dgate, dup, dwdc, grad = take(13)
    load_sem, w_sem, dwd_sem = take(3)
    kinds = []
    for name in "ab":
        k = Kind()
        k.name = name
        k.dd, k.s1, k.r1, k.s2, k.r2, k.m, k.v, k.w, k.nw, k.g = take(10)
        k.dd_s, k.dd_r, k.s1_s, k.s1_r, k.s2_s, k.s2_r = take(6)
        k.ax_s, k.ax_r, k.ah_s, k.ah_r, k.ad_s, k.ad_r, k.st_sem, k.out_sem = take(8)
        kinds.append(k)
    ka, kb = kinds
    kb.own, kb.own_sem = take(2)
    assert next(it, None) is None

    me = lax.axis_index("dp")
    chip, core = me // 2, me % 2
    other = 1 - core
    right, left, across = (chip + 1) % 4, (chip + 3) % 4, (chip + 2) % 4
    partner = chip * 2 + other
    to = (right * 2 + core, left * 2 + core)
    frm = (left, right)

    barrier = pltpu.get_barrier_semaphore()
    for peer in (partner, *to):
        pl.semaphore_signal(barrier, inc=1, device_id={"dp": peer}, device_id_type=MESH)
    pl.semaphore_wait(barrier, 3)

    def remote(src, dst, send, recv, peer):
        return pltpu.make_async_remote_copy(src_ref=src, dst_ref=dst, send_sem=send, recv_sem=recv,
                                            device_id={"dp": peer}, device_id_type=MESH)

    local = pltpu.make_async_copy
    aligned = lambda i, n: pl.ds(pl.multiple_of(i * n, n), n)

    ka.na, ka.r, ka.n, ka.half = 2, R, C, (2, R // 2, C)
    kb.na, kb.r, kb.n, kb.half = 1, PB, D, (1, PB, D // 2)
    ka.first, kb.first = 0, PIECES
    for k in kinds:
        k.where = lambda s, k=k: (1 - (s - k.first) // PIECES, (s - k.first) % PIECES)

    def own_a(s, y):
        return grad.at[s % 2, :, y, core]

    ka.tile = own_a
    kb.tile = lambda s, y: kb.own.at[s % 2, :, y]

    def out_a(s, j):
        layer, c = ka.where(s)
        return nw_a.at[layer, :, aligned(j, R), aligned(c, C)]

    def out_half_a(s, j, h):
        layer, c = ka.where(s)
        return nw_a.at[layer, :, pl.ds(pl.multiple_of(j * R + h * (R // 2), R // 2), R // 2), aligned(c, C)]

    def rows_b(j, p):
        return pl.ds(pl.multiple_of(j * RB + p * PB, PB), PB)

    def out_b(s, j):
        layer, p = kb.where(s)
        return nw_b.at[pl.ds(layer, 1), rows_b(j, p)]

    def out_half_b(s, j, h):
        layer, p = kb.where(s)
        return nw_b.at[pl.ds(layer, 1), rows_b(j, p), pl.ds(h * (D // 2), D // 2)]

    ka.out, ka.out_half, kb.out, kb.out_half = out_a, out_half_a, out_b, out_half_b
    ka.half_of = lambda ref, h: ref.at[:, pl.ds(h * (R // 2), R // 2), :]
    kb.half_of = lambda ref, h: ref.at[:, :, pl.ds(h * (D // 2), D // 2)]

    def state_copies(k, s):
        layer, c = k.where(s)
        if k is ka:
            cols = aligned(c, C)
            out = []
            for i, (w, m, v) in enumerate(((wg, mg, vg), (wu, mu, vu))):
                out += [local(w.at[layer, aligned(me, R), cols], k.w.at[i], k.st_sem.at[3 * i]),
                        local(m.at[layer, :, cols], k.m.at[i], k.st_sem.at[3 * i + 1]),
                        local(v.at[layer, :, cols], k.v.at[i], k.st_sem.at[3 * i + 2])]
            return out
        rows = aligned(c, PB)
        one = pl.ds(layer, 1)
        return [local(wd.at[one, rows_b(me, c)], k.w, k.st_sem.at[0]),
                local(md.at[one, rows], k.m, k.st_sem.at[1]), local(vd.at[one, rows], k.v, k.st_sem.at[2])]

    def g_out(k, s):
        layer, c = k.where(s)
        return g_a.at[layer, :, :, aligned(c, C)] if k is ka else g_b.at[pl.ds(layer, 1), aligned(c, PB)]

    def own_copy(k, s):
        return (local(k.nw.at[s % 2], k.out(s, me), k.out_sem.at[s % 2, 0]),
                local(k.g.at[s % 2], g_out(k, s), k.out_sem.at[s % 2, 1]))

    def dd_copy(k, s):
        return remote(grad.at[s % 2, :, :, other], k.dd.at[s % 2], k.dd_s.at[s % 2], k.dd_r.at[s % 2], partner)

    def s1_copy(k, s, h):
        return remote(k.half_of(k.s1.at[s % 2], h), k.r1.at[s % 2, h], k.s1_s.at[s % 2, h], k.s1_r.at[s % 2, h], to[h])

    def s2_copy(k, s, h):
        return remote(k.s2.at[s % 2, h], k.r2.at[s % 2, h], k.s2_s.at[s % 2, h], k.s2_r.at[s % 2, h], to[h])

    def ax_copy(k, s, h):
        return remote(k.nw.at[s % 2], k.out(s, me), k.ax_s.at[s % 4, h], k.ax_r.at[s % 4, h], to[h])

    def ax_wait(k, s, h):
        j = frm[h] * 2 + core
        return remote(k.out(s, j), k.out(s, j), k.ax_s.at[s % 4, h], k.ax_r.at[s % 4, h], to[h])

    def ah_copy(k, s, h):
        src = k.out_half(s, frm[h] * 2 + core, h)
        return remote(src, src, k.ah_s.at[s % 4, h], k.ah_r.at[s % 4, h], to[h])

    def ah_wait(k, s, h):
        src = k.out_half(s, across * 2 + core, h)
        return remote(src, src, k.ah_s.at[s % 4, h], k.ah_r.at[s % 4, h], to[h])

    def ad_copy(k, s, i):
        if i == 0:
            return remote(k.nw.at[s % 2], k.out(s, me), k.ad_s.at[s % 4, 0], k.ad_r.at[s % 4, 0], partner)
        y = (chip, left, right, across)[i]
        src = k.out(s, y * 2 + core)
        return remote(src, src, k.ad_s.at[s % 4, i], k.ad_r.at[s % 4, i], partner)

    def ad_wait(k, s, i):
        y = (chip, left, right, across)[i]
        src = k.out(s, y * 2 + other)
        return remote(src, src, k.ad_s.at[s % 4, i], k.ad_r.at[s % 4, i], partner)

    def blocks(k, body):
        rows, cols = k.half[1], k.half[2]
        for h in range(2):
            @pl.loop(0, rows // 16)
            def _(i):
                if k is ka:
                    cut = lambda ref: ref.at[:, pl.ds(pl.multiple_of(h * rows + i * 16, 16), 16), :]
                else:
                    cut = lambda ref: ref.at[:, pl.ds(pl.multiple_of(i * 16, 16), 16), pl.ds(h * cols, cols)]
                cut_half = lambda ref: ref.at[:, pl.ds(pl.multiple_of(i * 16, 16), 16), :]
                body(cut, cut_half, h)

    def stage_a(k, s):
        if k is ka:
            dd_copy(k, s).start()
            return
        layer, p = k.where(s)
        for y in range(4):
            local(dwd.at[layer, pl.ds((y * 2 + core) * PIECES + p, 1)], k.own.at[s % 2, :, y], k.own_sem.at[s % 2]).start()
            remote(dwd.at[layer, pl.ds((y * 2 + other) * PIECES + p, 1)], k.dd.at[s % 2, :, y],
                   k.dd_s.at[s % 2], k.dd_r.at[s % 2], partner).start()

    def dd_wait(k, s):
        return remote(k.dd.at[s % 2], k.dd.at[s % 2], k.dd_s.at[s % 2], k.dd_r.at[s % 2], partner)

    def stage_b(k, s):
        slot = s % 2
        dd_wait(k, s).wait_recv()
        if k is kb:
            local(k.own.at[slot], k.own.at[slot], k.own_sem.at[slot]).wait()
        mine, theirs = k.tile(s, across), k.dd.at[slot, :, across]

        def body(cut, cut_half, h):
            cut(k.s1.at[slot])[...] = wide_sum(cut(mine)[...], cut(theirs)[...]).astype(BF16)

        blocks(k, body)
        for h in range(2):
            s1_copy(k, s, h).start()
        for c in state_copies(k, s):
            c.start()

    def stage_c(k, s):
        slot = s % 2
        for h in range(2):
            s1_copy(k, s, h).wait_recv()
        for way in range(2):
            y = (right, left)[way]
            mine, theirs = k.tile(s, y), k.dd.at[slot, :, y]

            def body(cut, cut_half, h):
                parts = [cut(mine)[...], cut(theirs)[...]]
                if h == way:
                    parts.append(cut_half(k.r1.at[slot, way])[...])
                cut(k.s2.at[slot, way])[...] = wide_sum(*parts).astype(BF16)

            blocks(k, body)
            s2_copy(k, s, way).start()
        for h in range(2):
            s1_copy(k, s, h).wait_send()
        dd_wait(k, s).wait_send()

    def stage_d(k, s):
        slot = s % 2
        for c in state_copies(k, s):
            c.wait()
        for h in range(2):
            s2_copy(k, s, h).wait_recv()
        mine, theirs = k.tile(s, chip), k.dd.at[slot, :, chip]

        def body(cut, cut_half, h):
            g = wide_sum(cut(mine)[...], cut(theirs)[...], cut(k.r2.at[slot, 0])[...], cut(k.r2.at[slot, 1])[...]).astype(BF16)
            cut(k.g.at[slot])[...] = g
            m, v = new_moments(cut(k.m)[...], cut(k.v)[...], g.astype(F32))
            w = cut(k.w)[...].astype(F32)
            cut(k.nw.at[slot])[...] = (w - 0.02 * (m * lax.rsqrt(v + 1e-8) + 0.1 * w)).astype(BF16)

        blocks(k, body)
        for h in range(2):
            ax_copy(k, s, h).start()
        ad_copy(k, s, 0).start()
        for c in own_copy(k, s):
            c.start()
        for h in range(2):
            s2_copy(k, s, h).wait_send()

    def stage_e(k, s):
        for h in range(2):
            ax_wait(k, s, h).wait_recv()
            ah_copy(k, s, h).start()
            ad_copy(k, s, 1 + h).start()
        ad_wait(k, s, 0).wait_recv()
        for c in own_copy(k, s):
            c.wait()
        for h in range(2):
            ax_copy(k, s, h).wait_send()
        ad_copy(k, s, 0).wait_send()

    def stage_f(k, s):
        for h in range(2):
            ah_wait(k, s, h).wait_recv()
        ad_copy(k, s, 3).start()

    def stage_g(k, s):
        for i in range(1, 4):
            ad_wait(k, s, i).wait_recv()
        for h in range(2):
            ah_copy(k, s, h).wait_send()
        for i in range(1, 4):
            ad_copy(k, s, i).wait_send()

    def run(stage, k, s, base):
        @pl.when((s >= k.first) & (s < k.first + 2 * PIECES))
        def _():
            stage(k, s)

    def early(s, here):
        for k in here:
            run(stage_f, k, s - 2, 0)
        for k in here:
            run(stage_d, k, s - 1, 0)
        for k in here:
            run(stage_a, k, s, 0)

    def late(s, here):
        for k in here:
            run(stage_b, k, s, 0)

    def even(s, here):
        for k in here:
            run(stage_e, k, s - 1, 0)
        for k in here:
            run(stage_c, k, s, 0)
        for k in here:
            run(stage_g, k, s - 2, 0)

    def weight_copies(layer, c):
        return (local(wg.at[layer, :, aligned(c, C)], wgc, w_sem.at[0]), local(wu.at[layer, :, aligned(c, C)], wuc, w_sem.at[1]),
                local(wd.at[layer, aligned(c, C)], wdc, w_sem.at[2]))

    def dwd_copy(layer, c):
        return local(dwdc, dwd.at[layer, pl.ds(c * 8, 8)], dwd_sem)

    def chunks(layer, here):
        first = (1 - layer) * PIECES

        @pl.loop(0, PIECES)
        def _(c):
            s = c + first
            for copy in weight_copies(layer, c):
                copy.wait()

            def tokens(i):
                rows = aligned(i, TILE)
                gate = dot(a[rows, :], wgc[...])
                up = dot(a[rows, :], wuc[...])
                dact = dot(d[rows, :], wdc[...], 1, 1).astype(BF16).astype(F32)
                sig = jax.nn.sigmoid(gate)
                silu = gate * sig
                act[rows, :] = (silu * up).astype(BF16)
                dup[rows, :] = (dact * silu).astype(BF16)
                dgate[rows, :] = (dact * up * (sig * (1 + gate * (1 - sig)))).astype(BF16)
                if layer:
                    more = dot(dgate[rows, :], wgc[...], 1, 1) + dot(dup[rows, :], wuc[...], 1, 1)

                    @pl.when(c == 0)
                    def _():
                        da[rows, :] = more

                    @pl.when(c > 0)
                    def _():
                        da[rows, :] += more

            half = T // TILE // 2
            pl.loop(0, half)(tokens)
            even(s - 1, here)
            pl.loop(half, 2 * half)(tokens)

            @pl.when(c < PIECES - 1)
            def _():
                for copy in weight_copies(layer, c + 1):
                    copy.start()

            for i, by in enumerate((dgate, dup)):
                @pl.loop(0, 2)
                def _(j):
                    block = dot(at[aligned(j, D // 2), :], by[...]).astype(BF16)
                    grad[s % 2, i, pl.ds(j * 2, 2)] = block.reshape(2, 2, R, C)

            early(s, here)

            @pl.when(c > 0)
            def _():
                dwd_copy(layer, c - 1).wait()

            for j in range(4):
                block = dot(dt[j * (D // 4) : (j + 1) * (D // 4), :], act[...]).astype(BF16)
                dwdc[:, :, j * (D // 4) : (j + 1) * (D // 4)] = block.T.reshape(8, PB, D // 4)
            dwd_copy(layer, c).start()
            late(s, here)

        dwd_copy(layer, PIECES - 1).wait()

    top = [local(src, dst, load_sem.at[i]) for i, (src, dst) in enumerate(((a1, a), (a1t, at), (dy, d), (dyt, dt)))]
    for copy in (*top, *weight_copies(1, 0)):
        copy.start()
    for copy in top:
        copy.wait()
    chunks(1, (ka,))

    bring = local(h1, a, load_sem.at[0])
    bring.start()
    low_t = local(a0t, at, load_sem.at[1])
    low_t.start()
    for copy in weight_copies(0, 0):
        copy.start()
    bring.wait()

    @pl.loop(0, T // 256)
    def _(i):
        rows = aligned(i, 256)
        wide = a[rows, :].astype(F32)
        scale = lax.rsqrt(jnp.mean(wide * wide, -1, keepdims=True) + 1e-6)
        by = da[rows, :].astype(BF16).astype(F32)
        inner = jnp.mean(wide * by, -1, keepdims=True)
        through = (by * scale - wide * (inner * scale * scale * scale)).astype(BF16)
        total = d[rows, :] + through
        d[rows, :] = total
        dt[:, rows] = total.T

    low = local(a0, a, load_sem.at[0])
    low.start()
    low.wait()
    low_t.wait()
    chunks(0, (ka, kb))

    @pl.loop(2 * PIECES, 3 * PIECES + 3)
    def _(s):
        even(s - 1, (ka, kb))
        early(s, (ka, kb))
        late(s, (ka, kb))


def gathered_step(mesh, dims, operands):
    T, D, FF, C, R, RB, PB = dims
    hbm = pl.BlockSpec(memory_space=pl.ANY)
    vmem, dma = pltpu.VMEM, pltpu.SemaphoreType.DMA
    shapes = [vmem((T, D), BF16), vmem((D, T), BF16), vmem((T, D), BF16), vmem((D, T), BF16), vmem((T, D), F32)]
    shapes += [vmem((D, C), BF16), vmem((D, C), BF16), vmem((C, D), BF16)]
    shapes += [vmem((T, C), BF16)] * 3 + [vmem((8, PB, D), BF16), vmem((2, 2, 4, 2, R, C), BF16)]
    shapes += [dma((4,)), dma((3,)), dma]
    for na, r, n, half in ((2, R, C, (2, R // 2, C)), (1, PB, D, (1, PB, D // 2))):
        tile = (na, r, n)
        shapes += [vmem((2, na, 4, r, n), BF16), vmem((2, *tile), BF16), vmem((2, 2, *half), BF16), vmem((2, 2, *tile), BF16),
                   vmem((2, 2, *tile), BF16), vmem(tile, F32), vmem(tile, F32), vmem(tile, BF16), vmem((2, *tile), BF16),
                   vmem((2, *tile), BF16)]
        shapes += [dma((2,)), dma((2,)), dma((2, 2)), dma((2, 2)), dma((2, 2)), dma((2, 2))]
        shapes += [dma((4, 2)), dma((4, 2)), dma((4, 2)), dma((4, 2)), dma((4, 4)), dma((4, 4)), dma((6,)), dma((2, 2))]
    shapes += [vmem((2, 1, 4, PB, D), BF16), dma((2,))]
    out = lambda *s: jax.ShapeDtypeStruct(s, BF16)
    L = 2
    return pl.pallas_call(
        functools.partial(kernel, dims),
        out_shape=(out(L, 2, D, FF), out(L, FF, D), out(L, 2, R, FF), out(L, RB, D), out(L, 8 * PIECES, PB, D)),
        in_specs=[hbm] * len(operands),
        out_specs=(hbm,) * 5,
        scratch_shapes=shapes,
        compiler_params=pltpu.CompilerParams(collective_id=0, has_side_effects=True, vmem_limit_bytes=67_000_000),
        name="backward_and_update",
    )(*operands)


def solution(mesh):
    assert mesh.shape["dp"] == 8

    def body(x, dy, wg, wu, wd, mg, mu, md, vg, vu, vd):
        T, D = x.shape[1:]
        FF = wg.shape[2]
        dims = (T, D, FF, FF // PIECES, D // 8, FF // 8, FF // 8 // PIECES)
        x, dy = x[0], dy[0]
        a0 = norm(x)
        gate = dot(a0, wg[0])
        up = dot(a0, wu[0])
        h1 = x + dot((jax.nn.silu(gate) * up).astype(BF16), wd[0]).astype(BF16)
        a1 = norm(h1)
        operands = (a1, a1.T, dy, dy.T, h1, a0, a0.T, wg, wu, wd, mg, mu, md, vg, vu, vd)
        nw_a, nw_b, g_a, g_b, _ = gathered_step(mesh, dims, operands)
        g = [g_a[:, 0], g_a[:, 1], g_b]
        new = [new_moments(m, v, t.astype(F32)) for m, v, t in zip((mg, mu, md), (vg, vu, vd), g, strict=True)]
        return (nw_a[:, 0], nw_a[:, 1], nw_b, *(t[0] for t in new), *(t[1] for t in new))

    seq, rep, rows = P(("rep", "dp")), P(), P(None, "dp")
    return jax.shard_map(
        body, mesh=mesh, in_specs=(seq, seq, rep, rep, rep) + (rows,) * 6,
        out_specs=(P("rep"),) * 3 + (P("rep", "dp"),) * 6, check_vma=False)
```

```python
import functools

import jax
import jax.numpy as jnp
from jax import lax
from jax.experimental import pallas as pl
from jax.experimental.pallas import tpu as pltpu
from jax.sharding import PartitionSpec as P

F32, BF16 = jnp.float32, jnp.bfloat16
PIECES = 5
TILE, SMALL = 512, 256
MESH = pl.DeviceIdType.MESH


def dot(a, b, ca=1, cb=0):
    return lax.dot_general(a, b, (((ca,), (cb,)), ((), ())), preferred_element_type=F32)


def norm(h):
    wide = h.astype(F32)
    scale = lax.rsqrt(jnp.mean(wide * wide, -1, keepdims=True) + 1e-6)
    return (wide * scale).astype(BF16)


def new_moments(m, v, g):
    return 0.9 * m + 0.1 * g, 0.95 * v + 0.05 * g * g


class Kind:
    pass


def wide_sum(*parts):
    total = parts[0].astype(F32)
    for part in parts[1:]:
        total = total + part.astype(F32)
    return total


def kernel(dims, *refs):
    T, D, FF, C, R, RB, PB = dims
    it = iter(refs)
    take = lambda n: [next(it) for _ in range(n)]
    x, dy = take(2)
    wg, wu, wd, mg, mu, md, vg, vu, vd = take(9)
    nw_g, nw_u, nw_d, g_a, g_b, dwd, h1, kept = take(8)
    a, at, d, dt, da, wgu, wdc, act, dgu, dwdc, grad = take(11)
    load_sem, w_sem, dwd_sem, tile_sem = take(4)
    kinds = []
    for name in "ab":
        k = Kind()
        k.name = name
        k.dd, k.s1, k.r1, k.s2, k.r2, k.m, k.v, k.w, k.nw, k.g = take(10)
        k.dd_s, k.dd_r, k.s1_s, k.s1_r, k.s2_s, k.s2_r = take(6)
        k.ax_s, k.ax_r, k.ah_s, k.ah_r, k.ad_s, k.ad_r, k.st_sem, k.out_sem, k.free = take(9)
        kinds.append(k)
    ka, kb = kinds
    kb.own, kb.own_sem = take(2)
    assert next(it, None) is None

    me = lax.axis_index("dp")
    chip, core = lax.div(me, 2), lax.rem(me, 2)
    other = 1 - core
    right, left, across = lax.rem(chip + 1, 4), lax.rem(chip + 3, 4), lax.rem(chip + 2, 4)
    partner = chip * 2 + other
    to = (right * 2 + core, left * 2 + core)
    frm = (left, right)

    barrier = pltpu.get_barrier_semaphore()
    for peer in (partner, *to):
        pl.semaphore_signal(barrier, inc=1, device_id={"dp": peer}, device_id_type=MESH)

    def remote(src, dst, send, recv, peer):
        return pltpu.make_async_remote_copy(src_ref=src, dst_ref=dst, send_sem=send, recv_sem=recv,
                                            device_id={"dp": peer}, device_id_type=MESH)

    local = pltpu.make_async_copy
    aligned = lambda i, n: pl.ds(pl.multiple_of(i * n, n), n)

    ka.na, ka.r, ka.n, ka.half = 2, R, C, (2, R // 2, C)
    kb.na, kb.r, kb.n, kb.half = 1, PB, D, (1, PB, D // 2)
    ka.first, ka.gap = 0, 2 * PIECES
    kb.first, kb.gap = PIECES, 2 * PIECES

    class Job:
        def __init__(self, k, since):
            late = lax.div(since, k.gap)
            self.layer, self.piece = 1 - late, since - late * k.gap
            self.turn = self.piece + late * PIECES
            self.slot, self.mark = lax.rem(self.turn, 2), lax.rem(self.turn, 8)

    def own_a(s, y):
        return grad.at[s.slot, :, y, core]

    ka.tile = own_a
    kb.tile = lambda s, y: kb.own.at[s.slot, :, y]

    def rows_b(j, p):
        return pl.ds(pl.multiple_of(j * RB + p * PB, PB), PB)

    def out_a(s, j, h=None):
        layer, c = s.layer, s.piece
        rows = aligned(j, R) if h is None else pl.ds(pl.multiple_of(j * R + h * (R // 2), R // 2), R // 2)
        return [nw.at[layer, rows, aligned(c, C)] for nw in (nw_g, nw_u)]

    def out_b(s, j, h=None):
        layer, p = s.layer, s.piece
        one = pl.ds(layer, 1)
        return [nw_d.at[one, rows_b(j, p)] if h is None else nw_d.at[one, rows_b(j, p), pl.ds(h * (D // 2), D // 2)]]

    ka.out, kb.out = out_a, out_b
    ka.mine = lambda s: [ka.nw.at[s.slot, i] for i in range(2)]
    kb.mine = lambda s: [kb.nw.at[s.slot]]
    ka.half_of = lambda ref, h: ref.at[:, pl.ds(h * (R // 2), R // 2), :]
    kb.half_of = lambda ref, h: ref.at[:, :, pl.ds(h * (D // 2), D // 2)]

    def state_copies(k, s):
        layer, c = s.layer, s.piece
        if k is ka:
            cols = aligned(c, C)
            out = []
            for i, (w, m, v) in enumerate(((wg, mg, vg), (wu, mu, vu))):
                out += [local(w.at[layer, aligned(me, R), cols], k.w.at[i], k.st_sem.at[3 * i]),
                        local(m.at[layer, :, cols], k.m.at[i], k.st_sem.at[3 * i + 1]),
                        local(v.at[layer, :, cols], k.v.at[i], k.st_sem.at[3 * i + 2])]
            return out
        rows = aligned(c, PB)
        one = pl.ds(layer, 1)
        return [local(wd.at[one, rows_b(me, c)], k.w, k.st_sem.at[0]),
                local(md.at[one, rows], k.m, k.st_sem.at[1]), local(vd.at[one, rows], k.v, k.st_sem.at[2])]

    def g_out(k, s):
        layer, c = s.layer, s.piece
        return g_a.at[layer, :, :, aligned(c, C)] if k is ka else g_b.at[pl.ds(layer, 1), aligned(c, PB)]

    def own_copies(k, s):
        slot = s.slot
        return [local(src, dst, k.out_sem.at[slot, 0]) for src, dst in zip(k.mine(s), k.out(s, me), strict=True)] + [
            local(k.g.at[slot], g_out(k, s), k.out_sem.at[slot, 1])]

    def own_wait(k, s):
        slot = s.slot
        local(k.nw.at[slot], k.nw.at[slot], k.out_sem.at[slot, 0]).wait()
        local(k.g.at[slot], k.g.at[slot], k.out_sem.at[slot, 1]).wait()

    def dd_copy(k, s):
        return remote(grad.at[s.slot, :, :, other], k.dd.at[s.slot], k.dd_s.at[s.slot], k.dd_r.at[s.slot], partner)

    def s1_copy(k, s, h):
        return remote(k.half_of(k.s1.at[s.slot], h), k.r1.at[s.slot, h], k.s1_s.at[s.slot, h], k.s1_r.at[s.slot, h], to[h])

    def s2_copy(k, s, h):
        return remote(k.s2.at[s.slot, h], k.r2.at[s.slot, h], k.s2_s.at[s.slot, h], k.s2_r.at[s.slot, h], to[h])

    def whole(k, send, recv, peer):
        return remote(k.nw.at[0], k.nw.at[0], send, recv, peer)

    def half(k, h, send, recv, peer):
        return remote(k.half_of(k.nw.at[0], h), k.half_of(k.nw.at[0], h), send, recv, peer)

    def ax_start(k, s, h):
        for src, dst in zip(k.mine(s), k.out(s, me), strict=True):
            remote(src, dst, k.ax_s.at[s.mark, h], k.ax_r.at[s.mark, h], to[h]).start()

    def ax_wait(k, s, h):
        return whole(k, k.ax_s.at[s.mark, h], k.ax_r.at[s.mark, h], to[h])

    def ah_start(k, s, h):
        for src in k.out(s, frm[h] * 2 + core, h):
            remote(src, src, k.ah_s.at[s.mark, h], k.ah_r.at[s.mark, h], to[h]).start()

    def ah_wait(k, s, h):
        return half(k, h, k.ah_s.at[s.mark, h], k.ah_r.at[s.mark, h], to[h])

    def ad_start(k, s, i):
        dst = k.out(s, (chip, left, right, across)[i] * 2 + core)
        for src, dst in zip(k.mine(s) if i == 0 else dst, dst, strict=True):
            remote(src, dst, k.ad_s.at[s.mark, i], k.ad_r.at[s.mark, i], partner).start()

    def ad_wait(k, s, i):
        return whole(k, k.ad_s.at[s.mark, i], k.ad_r.at[s.mark, i], partner)

    def blocks(k, body):
        rows, cols = k.half[1], k.half[2]
        for h in range(2):
            @pl.loop(0, rows // 16)
            def _(i):
                if k is ka:
                    cut = lambda ref: ref.at[:, pl.ds(pl.multiple_of(h * rows + i * 16, 16), 16), :]
                else:
                    cut = lambda ref: ref.at[:, pl.ds(pl.multiple_of(i * 16, 16), 16), pl.ds(h * cols, cols)]
                cut_half = lambda ref: ref.at[:, pl.ds(pl.multiple_of(i * 16, 16), 16), :]
                body(cut, cut_half, h)

    def stage_a(k, s):
        @pl.when(s.turn >= 2)
        def _():
            pl.semaphore_wait(k.free, 1)

        if k is ka:
            dd_copy(k, s).start()
            return
        layer, p = s.layer, s.piece
        for y in range(4):
            local(dwd.at[layer, pl.ds((y * 2 + core) * PIECES + p, 1)], k.own.at[s.slot, :, y], k.own_sem.at[s.slot]).start()
            remote(dwd.at[layer, pl.ds((y * 2 + other) * PIECES + p, 1)], k.dd.at[s.slot, :, y],
                   k.dd_s.at[s.slot], k.dd_r.at[s.slot], partner).start()

    def dd_wait(k, s):
        return remote(k.dd.at[s.slot], k.dd.at[s.slot], k.dd_s.at[s.slot], k.dd_r.at[s.slot], partner)

    def stage_b(k, s):
        slot = s.slot
        dd_wait(k, s).wait_recv()
        if k is kb:
            local(k.own.at[slot], k.own.at[slot], k.own_sem.at[slot]).wait()
        mine, theirs = k.tile(s, across), k.dd.at[slot, :, across]

        def body(cut, cut_half, h):
            cut(k.s1.at[slot])[...] = wide_sum(cut(mine)[...], cut(theirs)[...]).astype(BF16)

        blocks(k, body)
        for h in range(2):
            s1_copy(k, s, h).start()

    def stage_c(k, s):
        slot = s.slot
        for c in state_copies(k, s):
            c.start()
        for h in range(2):
            s1_copy(k, s, h).wait_recv()
        for way in range(2):
            y = (right, left)[way]
            mine, theirs = k.tile(s, y), k.dd.at[slot, :, y]

            def body(cut, cut_half, h):
                parts = [cut(mine)[...], cut(theirs)[...]]
                if h == way:
                    parts.append(cut_half(k.r1.at[slot, way])[...])
                cut(k.s2.at[slot, way])[...] = wide_sum(*parts).astype(BF16)

            blocks(k, body)
            s2_copy(k, s, way).start()
        for h in range(2):
            s1_copy(k, s, h).wait_send()
        dd_wait(k, s).wait_send()

    def stage_d(k, s):
        slot = s.slot
        for c in state_copies(k, s):
            c.wait()
        for h in range(2):
            s2_copy(k, s, h).wait_recv()
        mine, theirs = k.tile(s, chip), k.dd.at[slot, :, chip]

        def body(cut, cut_half, h):
            g = wide_sum(cut(mine)[...], cut(theirs)[...], cut(k.r2.at[slot, 0])[...], cut(k.r2.at[slot, 1])[...]).astype(BF16)
            cut(k.g.at[slot])[...] = g
            m, v = new_moments(cut(k.m)[...], cut(k.v)[...], g.astype(F32))
            w = cut(k.w)[...].astype(F32)
            cut(k.nw.at[slot])[...] = (w - 0.02 * (m * lax.rsqrt(v + 1e-8) + 0.1 * w)).astype(BF16)

        blocks(k, body)

        @pl.when(s.turn < 2 * PIECES - 2)
        def _():
            pl.semaphore_signal(k.free, inc=1, device_id={"dp": partner}, device_id_type=MESH)

        for h in range(2):
            ax_start(k, s, h)
        ad_start(k, s, 0)
        for c in own_copies(k, s):
            c.start()
        for h in range(2):
            s2_copy(k, s, h).wait_send()

    def stage_e(k, s):
        for h in range(2):
            ax_wait(k, s, h).wait_recv()
            ah_start(k, s, h)
            ad_start(k, s, 1 + h)
        ad_wait(k, s, 0).wait_recv()
        own_wait(k, s)
        for h in range(2):
            ax_wait(k, s, h).wait_send()
        ad_wait(k, s, 0).wait_send()

    def stage_f(k, s):
        for h in range(2):
            ah_wait(k, s, h).wait_recv()
        ad_start(k, s, 3)

    def stage_g(k, s):
        for i in range(1, 4):
            ad_wait(k, s, i).wait_recv()
        for h in range(2):
            ah_wait(k, s, h).wait_send()
        for i in range(1, 4):
            ad_wait(k, s, i).wait_send()

    def run(stage, k, s):
        since = s - k.first

        @pl.when((since >= 0) & (since < 2 * k.gap) & (lax.rem(since, k.gap) < PIECES))
        def _():
            stage(k, Job(k, since))

    def before(s):
        for stage, lag in ((stage_e, 3), (stage_d, 2), (stage_c, 1)):
            for k in kinds:
                run(stage, k, s - lag)

    def send(s):
        for k in kinds:
            run(stage_a, k, s)

    def after(s):
        for stage, lag in ((stage_f, 4), (stage_b, 0), (stage_g, 5)):
            for k in kinds:
                run(stage, k, s - lag)

    def up_copies(layer, c):
        cols = aligned(c, C)
        return (local(wg.at[layer, :, cols], wgu.at[lax.rem(c, 2), :, pl.ds(0, C)], w_sem.at[lax.rem(c, 2), 0]),
                local(wu.at[layer, :, cols], wgu.at[lax.rem(c, 2), :, pl.ds(C, C)], w_sem.at[lax.rem(c, 2), 1]))

    def down_copy(layer, c):
        return local(wd.at[layer, aligned(c, C)], wdc, w_sem.at[0, 2])

    def start(copies):
        for copy in copies:
            copy.start()

    def wait(copies):
        for copy in copies:
            copy.wait()

    def next_up(layer, c):
        @pl.when(c < PIECES - 1)
        def _():
            start(up_copies(layer, c + 1))

    def put(ref, c, rows, value):
        @pl.when(c == 0)
        def _():
            ref[rows, :] = value

        @pl.when(c > 0)
        def _():
            ref[rows, :] += value

    def dwd_copy(layer, c):
        return local(dwdc, dwd.at[layer, pl.ds(c * 8, 8)], dwd_sem)

    def dgu_copy(c, rows, back, sem):
        there = kept.at[c, rows]
        return local(there, dgu.at[rows], sem) if back else local(dgu.at[rows], there, sem)

    every = pl.ds(0, T)
    wide_rows = lambda ref: ref.at[:, pl.ds(0, D)]

    def chunks(layer):
        first = (1 - layer) * 2 * PIECES

        @pl.loop(0, PIECES)
        def _(c):
            s = c + first
            wait(up_copies(layer, c))
            next_up(layer, c)
            down_copy(layer, c).wait()
            if layer:
                @pl.when(c > 0)
                def _():
                    dgu_copy(c, every, False, load_sem.at[2]).wait()

            def tokens(i):
                rows = aligned(i, SMALL)
                gu = dot(a[rows, :], wgu[lax.rem(c, 2)])
                dact = dot(d[rows, :], wdc[...], 1, 1).astype(BF16).astype(F32)
                gate, up = gu[:, :C], gu[:, C:]
                sig = jax.nn.sigmoid(gate)
                silu = gate * sig
                act[rows, :] = (silu * up).astype(BF16)
                dgu[rows, :C] = (dact * up * (sig * (1 + gate * (1 - sig)))).astype(BF16)
                dgu[rows, C:] = (dact * silu).astype(BF16)

            pl.loop(0, T // SMALL // 2)(tokens)
            before(s)
            pl.loop(T // SMALL // 2, T // SMALL)(tokens)
            if layer:
                dgu_copy(c, every, False, load_sem.at[2]).start()

            @pl.when(c < PIECES - 1)
            def _():
                down_copy(layer, c + 1).start()

            @pl.loop(0, 2)
            def _(j):
                block = dot(at[aligned(j, D // 2), :], dgu[...]).astype(BF16)
                for i in range(2):
                    grad[lax.rem(c + (1 - layer) * PIECES, 2), i, pl.ds(j * 2, 2)] = block[:, i * C : (i + 1) * C].reshape(2, 2, R, C)

            send(s)

            @pl.when(c > 0)
            def _():
                dwd_copy(layer, c - 1).wait()

            for j in range(4):
                block = dot(dt[j * (D // 4) : (j + 1) * (D // 4), :], act[...]).astype(BF16)
                dwdc[:, :, j * (D // 4) : (j + 1) * (D // 4)] = block.T.reshape(8, PB, D // 4)
            dwd_copy(layer, c).start()
            after(s)

        dwd_copy(layer, PIECES - 1).wait()

    bring = [local(x, a, load_sem.at[0]), local(dy, d, load_sem.at[1]), local(x, wide_rows(dgu), load_sem.at[2])]
    start(bring)
    start(up_copies(0, 0))
    down_copy(0, 0).start()
    wait(bring[:1])

    @pl.loop(0, T // 128)
    def _(i):
        rows = aligned(i, 128)
        a[rows, :] = norm(a[rows, :])

    @pl.loop(0, PIECES)
    def _(c):
        wait(up_copies(0, c))
        next_up(0, c)
        down_copy(0, c).wait()

        @pl.loop(0, T // TILE)
        def _(i):
            rows = aligned(i, TILE)
            gu = dot(a[rows, :], wgu[lax.rem(c, 2)])
            gate = gu[:, :C]
            act[rows, :] = (gate * jax.nn.sigmoid(gate) * gu[:, C:]).astype(BF16)
            put(da, c, rows, dot(act[rows, :], wdc[...]))

        @pl.when(c < PIECES - 1)
        def _():
            down_copy(0, c + 1).start()

    start(up_copies(1, 0))
    down_copy(1, 0).start()
    wait(bring[1:])

    @pl.loop(0, T // 128)
    def _(i):
        rows = aligned(i, 128)
        h = dgu[rows, :D] + da[rows, :].astype(BF16)
        dgu[rows, :D] = h
        low = norm(h)
        a[rows, :] = low
        at[:, rows] = low.T
        dt[:, rows] = d[rows, :].T

    keep = local(wide_rows(dgu), h1, load_sem.at[0])
    keep.start()
    pl.semaphore_wait(barrier, 3)
    keep.wait()

    chunks(1)

    bring = local(h1, a, load_sem.at[0])
    bring.start()
    start(up_copies(1, 0))
    dgu_copy(PIECES - 1, every, False, load_sem.at[2]).wait()
    tiles = T // TILE

    @pl.loop(0, tiles)
    def _(i):
        dgu_copy(0, aligned(i, TILE), True, tile_sem.at[i]).start()

    @pl.loop(0, PIECES)
    def _(c):
        s = c + PIECES
        wait(up_copies(1, c))
        next_up(1, c)

        def tokens(i):
            rows = aligned(i, TILE)
            dgu_copy(c, rows, True, tile_sem.at[i]).wait()
            put(da, c, rows, dot(dgu[rows, :], wgu[lax.rem(c, 2)], 1, 1))

            @pl.when(c < PIECES - 1)
            def _():
                dgu_copy(c + 1, rows, True, tile_sem.at[i]).start()

        before(s)
        send(s)
        pl.loop(0, tiles)(tokens)
        after(s)

    again = local(x, wide_rows(dgu), load_sem.at[1])
    again.start()
    start(up_copies(0, 0))
    down_copy(0, 0).start()
    bring.wait()

    @pl.loop(0, T // 128)
    def _(i):
        rows = aligned(i, 128)
        wide = a[rows, :].astype(F32)
        scale = lax.rsqrt(jnp.mean(wide * wide, -1, keepdims=True) + 1e-6)
        by = da[rows, :].astype(BF16).astype(F32)
        inner = jnp.mean(wide * by, -1, keepdims=True)
        total = d[rows, :] + (by * scale - wide * (inner * scale * scale * scale)).astype(BF16)
        d[rows, :] = total
        dt[:, rows] = total.T

    again.wait()

    @pl.loop(0, T // 128)
    def _(i):
        rows = aligned(i, 128)
        low = norm(dgu[rows, :D])
        a[rows, :] = low
        at[:, rows] = low.T

    chunks(0)

    @pl.loop(3 * PIECES, 4 * PIECES + 5)
    def _(s):
        before(s)
        send(s)
        after(s)


def gathered_step(mesh, dims, operands):
    T, D, FF, C, R, RB, PB = dims
    hbm = pl.BlockSpec(memory_space=pl.ANY)
    vmem, dma = pltpu.VMEM, pltpu.SemaphoreType.DMA
    shapes = [vmem((T, D), BF16), vmem((D, T), BF16), vmem((T, D), BF16), vmem((D, T), BF16), vmem((T, D), F32)]
    shapes += [vmem((2, D, 2 * C), BF16), vmem((C, D), BF16), vmem((T, C), BF16), vmem((T, 2 * C), BF16)]
    shapes += [vmem((8, PB, D), BF16), vmem((2, 2, 4, 2, R, C), BF16)]
    shapes += [dma((3,)), dma((2, 3)), dma, dma((T // TILE,))]
    for na, r, n, half in ((2, R, C, (2, R // 2, C)), (1, PB, D, (1, PB, D // 2))):
        tile = (na, r, n)
        shapes += [vmem((2, na, 4, r, n), BF16), vmem((2, *tile), BF16), vmem((2, 2, *half), BF16), vmem((2, 2, *tile), BF16),
                   vmem((2, 2, *tile), BF16), vmem(tile, F32), vmem(tile, F32), vmem(tile, BF16), vmem((2, *tile), BF16),
                   vmem((2, *tile), BF16)]
        shapes += [dma((2,)), dma((2,)), dma((2, 2)), dma((2, 2)), dma((2, 2)), dma((2, 2))]
        shapes += [dma((8, 2)), dma((8, 2)), dma((8, 2)), dma((8, 2)), dma((8, 4)), dma((8, 4)), dma((6,)), dma((2, 2)),
                   pltpu.SemaphoreType.REGULAR]
    shapes += [vmem((2, 1, 4, PB, D), BF16), dma((2,))]
    out = lambda *s: jax.ShapeDtypeStruct(s, BF16)
    L = 2
    return pl.pallas_call(
        functools.partial(kernel, dims),
        out_shape=(out(L, D, FF), out(L, D, FF), out(L, FF, D), out(L, 2, R, FF), out(L, RB, D), out(L, 8 * PIECES, PB, D),
                   out(T, D), out(PIECES, T, 2 * C)),
        in_specs=[hbm] * len(operands),
        out_specs=(hbm,) * 8,
        scratch_shapes=shapes,
        compiler_params=pltpu.CompilerParams(collective_id=0, has_side_effects=True, vmem_limit_bytes=67_000_000),
        name="step",
    )(*operands)


def solution(mesh):
    assert mesh.shape["dp"] == 8

    def body(x, dy, wg, wu, wd, mg, mu, md, vg, vu, vd):
        T, D = x.shape[1:]
        FF = wg.shape[2]
        dims = (T, D, FF, FF // PIECES, D // 8, FF // 8, FF // 8 // PIECES)
        nw_g, nw_u, nw_d, g_a, g_b, *_ = gathered_step(mesh, dims, (x[0], dy[0], wg, wu, wd, mg, mu, md, vg, vu, vd))
        g = [g_a[:, 0], g_a[:, 1], g_b]
        new = [new_moments(m, v, t.astype(F32)) for m, v, t in zip((mg, mu, md), (vg, vu, vd), g, strict=True)]
        return (nw_g, nw_u, nw_d, *(t[0] for t in new), *(t[1] for t in new))

    seq, rep, rows = P(("rep", "dp")), P(), P(None, "dp")
    return jax.shard_map(
        body, mesh=mesh, in_specs=(seq, seq, rep, rep, rep) + (rows,) * 6,
        out_specs=(P("rep"),) * 3 + (P("rep", "dp"),) * 6, check_vma=False)
```

```python
import functools

import jax
import jax.numpy as jnp
from jax import lax
from jax.experimental import pallas as pl
from jax.experimental.pallas import tpu as pltpu
from jax.sharding import PartitionSpec as P

F32, BF16 = jnp.float32, jnp.bfloat16
PIECES = 5
TILE, SMALL = 512, 256
MESH = pl.DeviceIdType.MESH


def dot(a, b, ca=1, cb=0):
    return lax.dot_general(a, b, (((ca,), (cb,)), ((), ())), preferred_element_type=F32)


def norm(h):
    wide = h.astype(F32)
    scale = lax.rsqrt(jnp.mean(wide * wide, -1, keepdims=True) + 1e-6)
    return (wide * scale).astype(BF16)


def new_moments(m, v, g):
    return 0.9 * m + 0.1 * g, 0.95 * v + 0.05 * g * g


class Kind:
    pass


def wide_sum(*parts):
    total = parts[0].astype(F32)
    for part in parts[1:]:
        total = total + part.astype(F32)
    return total


def kernel(dims, *refs):
    T, D, FF, C, R, RB, PB = dims
    it = iter(refs)
    take = lambda n: [next(it) for _ in range(n)]
    x, dy = take(2)
    wg, wu, wd, mg, mu, md, vg, vu, vd = take(9)
    nw_g, nw_u, nw_d, g_a, g_b, dwd, h1, kept = take(8)
    a, at, d, dt, da, wgu, wdc, act, dgu, dwdc, grad = take(11)
    load_sem, w_sem, dwd_sem, tile_sem = take(4)
    kinds = []
    for name in "ab":
        k = Kind()
        k.name = name
        k.dd, k.s1, k.r1, k.s2, k.r2, k.m, k.v, k.w, k.nw, k.g = take(10)
        k.dd_s, k.dd_r, k.s1_s, k.s1_r, k.s2_s, k.s2_r = take(6)
        k.ax_s, k.ax_r, k.ah_s, k.ah_r, k.ad_s, k.ad_r, k.st_sem, k.out_sem, k.free = take(9)
        kinds.append(k)
    ka, kb = kinds
    kb.own, kb.own_sem = take(2)
    assert next(it, None) is None

    me = lax.axis_index("dp")
    chip, core = lax.div(me, 2), lax.rem(me, 2)
    other = 1 - core
    right, left, across = lax.rem(chip + 1, 4), lax.rem(chip + 3, 4), lax.rem(chip + 2, 4)
    partner = chip * 2 + other
    to = (right * 2 + core, left * 2 + core)
    frm = (left, right)

    barrier = pltpu.get_barrier_semaphore()
    for peer in (partner, *to):
        pl.semaphore_signal(barrier, inc=1, device_id={"dp": peer}, device_id_type=MESH)

    def remote(src, dst, send, recv, peer):
        return pltpu.make_async_remote_copy(src_ref=src, dst_ref=dst, send_sem=send, recv_sem=recv,
                                            device_id={"dp": peer}, device_id_type=MESH)

    local = pltpu.make_async_copy
    aligned = lambda i, n: pl.ds(pl.multiple_of(i * n, n), n)

    ka.na, ka.r, ka.n, ka.half = 2, R, C, (2, R // 2, C)
    kb.na, kb.r, kb.n, kb.half = 1, PB, D, (1, PB, D // 2)
    ka.first, ka.gap = 0, 2 * PIECES
    kb.first, kb.gap = PIECES, 2 * PIECES

    class Job:
        def __init__(self, k, since):
            late = lax.div(since, k.gap)
            self.layer, self.piece = 1 - late, since - late * k.gap
            self.turn = self.piece + late * PIECES
            self.slot, self.mark = lax.rem(self.turn, 2), lax.rem(self.turn, 8)

    def own_a(s, y):
        return grad.at[s.slot, :, y, core]

    ka.tile = own_a
    kb.tile = lambda s, y: kb.own.at[s.slot, :, y]

    def rows_b(j, p):
        return pl.ds(pl.multiple_of(j * RB + p * PB, PB), PB)

    def out_a(s, j, h=None):
        layer, c = s.layer, s.piece
        rows = aligned(j, R) if h is None else pl.ds(pl.multiple_of(j * R + h * (R // 2), R // 2), R // 2)
        return [nw.at[layer, rows, aligned(c, C)] for nw in (nw_g, nw_u)]

    def out_b(s, j, h=None):
        layer, p = s.layer, s.piece
        one = pl.ds(layer, 1)
        return [nw_d.at[one, rows_b(j, p)] if h is None else nw_d.at[one, rows_b(j, p), pl.ds(h * (D // 2), D // 2)]]

    ka.out, kb.out = out_a, out_b
    ka.mine = lambda s: [ka.nw.at[s.slot, i] for i in range(2)]
    kb.mine = lambda s: [kb.nw.at[s.slot]]
    ka.half_of = lambda ref, h: ref.at[:, pl.ds(h * (R // 2), R // 2), :]
    kb.half_of = lambda ref, h: ref.at[:, :, pl.ds(h * (D // 2), D // 2)]

    def state_copies(k, s):
        layer, c = s.layer, s.piece
        if k is ka:
            cols = aligned(c, C)
            out = []
            for i, (w, m, v) in enumerate(((wg, mg, vg), (wu, mu, vu))):
                out += [local(w.at[layer, aligned(me, R), cols], k.w.at[i], k.st_sem.at[3 * i]),
                        local(m.at[layer, :, cols], k.m.at[i], k.st_sem.at[3 * i + 1]),
                        local(v.at[layer, :, cols], k.v.at[i], k.st_sem.at[3 * i + 2])]
            return out
        rows = aligned(c, PB)
        one = pl.ds(layer, 1)
        return [local(wd.at[one, rows_b(me, c)], k.w, k.st_sem.at[0]),
                local(md.at[one, rows], k.m, k.st_sem.at[1]), local(vd.at[one, rows], k.v, k.st_sem.at[2])]

    def g_out(k, s):
        layer, c = s.layer, s.piece
        return g_a.at[layer, :, :, aligned(c, C)] if k is ka else g_b.at[pl.ds(layer, 1), aligned(c, PB)]

    def own_copies(k, s):
        slot = s.slot
        return [local(src, dst, k.out_sem.at[slot, 0]) for src, dst in zip(k.mine(s), k.out(s, me), strict=True)] + [
            local(k.g.at[slot], g_out(k, s), k.out_sem.at[slot, 1])]

    def own_wait(k, s):
        slot = s.slot
        local(k.nw.at[slot], k.nw.at[slot], k.out_sem.at[slot, 0]).wait()
        local(k.g.at[slot], k.g.at[slot], k.out_sem.at[slot, 1]).wait()

    def dd_copy(k, s):
        return remote(grad.at[s.slot, :, :, other], k.dd.at[s.slot], k.dd_s.at[s.slot], k.dd_r.at[s.slot], partner)

    def s1_copy(k, s, h):
        return remote(k.half_of(k.s1.at[s.slot], h), k.r1.at[s.slot, h], k.s1_s.at[s.slot, h], k.s1_r.at[s.slot, h], to[h])

    def s2_copy(k, s, h):
        return remote(k.s2.at[s.slot, h], k.r2.at[s.slot, h], k.s2_s.at[s.slot, h], k.s2_r.at[s.slot, h], to[h])

    def whole(k, send, recv, peer):
        return remote(k.nw.at[0], k.nw.at[0], send, recv, peer)

    def half(k, h, send, recv, peer):
        return remote(k.half_of(k.nw.at[0], h), k.half_of(k.nw.at[0], h), send, recv, peer)

    def ax_start(k, s, h):
        for src, dst in zip(k.mine(s), k.out(s, me), strict=True):
            remote(src, dst, k.ax_s.at[s.mark, h], k.ax_r.at[s.mark, h], to[h]).start()

    def ax_wait(k, s, h):
        return whole(k, k.ax_s.at[s.mark, h], k.ax_r.at[s.mark, h], to[h])

    def ah_start(k, s, h):
        for src in k.out(s, frm[h] * 2 + core, h):
            remote(src, src, k.ah_s.at[s.mark, h], k.ah_r.at[s.mark, h], to[h]).start()

    def ah_wait(k, s, h):
        return half(k, h, k.ah_s.at[s.mark, h], k.ah_r.at[s.mark, h], to[h])

    def ad_start(k, s, i):
        dst = k.out(s, (chip, left, right, across)[i] * 2 + core)
        for src, dst in zip(k.mine(s) if i == 0 else dst, dst, strict=True):
            remote(src, dst, k.ad_s.at[s.mark, i], k.ad_r.at[s.mark, i], partner).start()

    def ad_wait(k, s, i):
        return whole(k, k.ad_s.at[s.mark, i], k.ad_r.at[s.mark, i], partner)

    def blocks(k, body):
        rows, cols = k.half[1], k.half[2]
        for h in range(2):
            @pl.loop(0, rows // 16)
            def _(i):
                if k is ka:
                    cut = lambda ref: ref.at[:, pl.ds(pl.multiple_of(h * rows + i * 16, 16), 16), :]
                else:
                    cut = lambda ref: ref.at[:, pl.ds(pl.multiple_of(i * 16, 16), 16), pl.ds(h * cols, cols)]
                cut_half = lambda ref: ref.at[:, pl.ds(pl.multiple_of(i * 16, 16), 16), :]
                body(cut, cut_half, h)

    def stage_a(k, s):
        @pl.when(s.turn >= 2)
        def _():
            pl.semaphore_wait(k.free, 1)

        if k is ka:
            dd_copy(k, s).start()
            return
        layer, p = s.layer, s.piece
        for y in range(4):
            local(dwd.at[layer, pl.ds((y * 2 + core) * PIECES + p, 1)], k.own.at[s.slot, :, y], k.own_sem.at[s.slot]).start()
            remote(dwd.at[layer, pl.ds((y * 2 + other) * PIECES + p, 1)], k.dd.at[s.slot, :, y],
                   k.dd_s.at[s.slot], k.dd_r.at[s.slot], partner).start()

    def dd_wait(k, s):
        return remote(k.dd.at[s.slot], k.dd.at[s.slot], k.dd_s.at[s.slot], k.dd_r.at[s.slot], partner)

    def stage_b(k, s):
        slot = s.slot
        dd_wait(k, s).wait_recv()
        if k is kb:
            local(k.own.at[slot], k.own.at[slot], k.own_sem.at[slot]).wait()
        mine, theirs = k.tile(s, across), k.dd.at[slot, :, across]

        def body(cut, cut_half, h):
            cut(k.s1.at[slot])[...] = wide_sum(cut(mine)[...], cut(theirs)[...]).astype(BF16)

        blocks(k, body)
        for h in range(2):
            s1_copy(k, s, h).start()

    def stage_c(k, s):
        slot = s.slot
        for c in state_copies(k, s):
            c.start()
        for h in range(2):
            s1_copy(k, s, h).wait_recv()
        for way in range(2):
            y = (right, left)[way]
            mine, theirs = k.tile(s, y), k.dd.at[slot, :, y]

            def body(cut, cut_half, h):
                parts = [cut(mine)[...], cut(theirs)[...]]
                if h == way:
                    parts.append(cut_half(k.r1.at[slot, way])[...])
                cut(k.s2.at[slot, way])[...] = wide_sum(*parts).astype(BF16)

            blocks(k, body)
            s2_copy(k, s, way).start()
        for h in range(2):
            s1_copy(k, s, h).wait_send()
        dd_wait(k, s).wait_send()

    def stage_d(k, s):
        slot = s.slot
        for c in state_copies(k, s):
            c.wait()
        for h in range(2):
            s2_copy(k, s, h).wait_recv()
        mine, theirs = k.tile(s, chip), k.dd.at[slot, :, chip]

        def body(cut, cut_half, h):
            g = wide_sum(cut(mine)[...], cut(theirs)[...], cut(k.r2.at[slot, 0])[...], cut(k.r2.at[slot, 1])[...]).astype(BF16)
            cut(k.g.at[slot])[...] = g
            m, v = new_moments(cut(k.m)[...], cut(k.v)[...], g.astype(F32))
            w = cut(k.w)[...].astype(F32)
            cut(k.nw.at[slot])[...] = (w - 0.02 * (m * lax.rsqrt(v + 1e-8) + 0.1 * w)).astype(BF16)

        blocks(k, body)

        @pl.when(s.turn < 2 * PIECES - 2)
        def _():
            pl.semaphore_signal(k.free, inc=1, device_id={"dp": partner}, device_id_type=MESH)

        for h in range(2):
            ax_start(k, s, h)
        ad_start(k, s, 0)
        for c in own_copies(k, s):
            c.start()
        for h in range(2):
            s2_copy(k, s, h).wait_send()

    def stage_e(k, s):
        for h in range(2):
            ax_wait(k, s, h).wait_recv()
            ah_start(k, s, h)
            ad_start(k, s, 1 + h)
        ad_wait(k, s, 0).wait_recv()
        own_wait(k, s)
        for h in range(2):
            ax_wait(k, s, h).wait_send()
        ad_wait(k, s, 0).wait_send()

    def stage_f(k, s):
        for h in range(2):
            ah_wait(k, s, h).wait_recv()
        ad_start(k, s, 3)

    def stage_g(k, s):
        for i in range(1, 4):
            ad_wait(k, s, i).wait_recv()
        for h in range(2):
            ah_wait(k, s, h).wait_send()
        for i in range(1, 4):
            ad_wait(k, s, i).wait_send()

    def run(stage, k, s):
        since = s - k.first

        @pl.when((since >= 0) & (since < 2 * k.gap) & (lax.rem(since, k.gap) < PIECES))
        def _():
            stage(k, Job(k, since))

    def before(s):
        for stage, lag in ((stage_e, 3), (stage_d, 2), (stage_c, 1)):
            for k in kinds:
                run(stage, k, s - lag)

    def send(s):
        for k in kinds:
            run(stage_a, k, s)

    def after(s):
        for stage, lag in ((stage_f, 4), (stage_b, 0), (stage_g, 5)):
            for k in kinds:
                run(stage, k, s - lag)

    def up_copies(layer, c):
        cols = aligned(c, C)
        return (local(wg.at[layer, :, cols], wgu.at[lax.rem(c, 2), :, pl.ds(0, C)], w_sem.at[lax.rem(c, 2), 0]),
                local(wu.at[layer, :, cols], wgu.at[lax.rem(c, 2), :, pl.ds(C, C)], w_sem.at[lax.rem(c, 2), 1]))

    def down_copy(layer, c):
        return local(wd.at[layer, aligned(c, C)], wdc, w_sem.at[0, 2])

    def start(copies):
        for copy in copies:
            copy.start()

    def wait(copies):
        for copy in copies:
            copy.wait()

    def next_up(layer, c):
        @pl.when(c < PIECES - 1)
        def _():
            start(up_copies(layer, c + 1))

    def put(ref, c, rows, value):
        @pl.when(c == 0)
        def _():
            ref[rows, :] = value

        @pl.when(c > 0)
        def _():
            ref[rows, :] += value

    def dwd_copy(layer, c):
        return local(dwdc, dwd.at[layer, pl.ds(c * 8, 8)], dwd_sem)

    def dgu_copy(c, rows, back, sem):
        there = kept.at[c, rows]
        return local(there, dgu.at[rows], sem) if back else local(dgu.at[rows], there, sem)

    every = pl.ds(0, T)
    wide_rows = lambda ref: ref.at[:, pl.ds(0, D)]

    def chunks(layer):
        first = (1 - layer) * 2 * PIECES

        @pl.loop(0, PIECES)
        def _(c):
            s = c + first
            wait(up_copies(layer, c))
            next_up(layer, c)
            down_copy(layer, c).wait()
            if layer:
                @pl.when(c > 0)
                def _():
                    dgu_copy(c, every, False, load_sem.at[2]).wait()

            def tokens(i):
                rows = aligned(i, SMALL)
                gu = dot(a[rows, :], wgu[lax.rem(c, 2)])
                dact = dot(d[rows, :], wdc[...], 1, 1).astype(BF16).astype(F32)
                gate, up = gu[:, :C], gu[:, C:]
                sig = jax.nn.sigmoid(gate)
                silu = gate * sig
                act[rows, :] = (silu * up).astype(BF16)
                dgu[rows, :C] = (dact * up * (sig * (1 + gate * (1 - sig)))).astype(BF16)
                dgu[rows, C:] = (dact * silu).astype(BF16)

            pl.loop(0, T // SMALL)(tokens)
            if layer:
                dgu_copy(c, every, False, load_sem.at[2]).start()

            @pl.when(c < PIECES - 1)
            def _():
                down_copy(layer, c + 1).start()

            before(s)

            @pl.loop(0, 2)
            def _(j):
                block = dot(at[aligned(j, D // 2), :], dgu[...]).astype(BF16)
                for i in range(2):
                    grad[lax.rem(c + (1 - layer) * PIECES, 2), i, pl.ds(j * 2, 2)] = block[:, i * C : (i + 1) * C].reshape(2, 2, R, C)

            send(s)

            @pl.when(c > 0)
            def _():
                dwd_copy(layer, c - 1).wait()

            for j in range(4):
                block = dot(dt[j * (D // 4) : (j + 1) * (D // 4), :], act[...]).astype(BF16)
                dwdc[:, :, j * (D // 4) : (j + 1) * (D // 4)] = block.T.reshape(8, PB, D // 4)
            dwd_copy(layer, c).start()
            after(s)

        dwd_copy(layer, PIECES - 1).wait()

    bring = [local(x, a, load_sem.at[0]), local(dy, d, load_sem.at[1]), local(x, wide_rows(dgu), load_sem.at[2])]
    start(bring)
    start(up_copies(0, 0))
    down_copy(0, 0).start()
    wait(bring[:1])

    @pl.loop(0, T // 128)
    def _(i):
        rows = aligned(i, 128)
        a[rows, :] = norm(a[rows, :])

    @pl.loop(0, PIECES)
    def _(c):
        wait(up_copies(0, c))
        next_up(0, c)
        down_copy(0, c).wait()

        @pl.loop(0, T // TILE)
        def _(i):
            rows = aligned(i, TILE)
            gu = dot(a[rows, :], wgu[lax.rem(c, 2)])
            gate = gu[:, :C]
            act[rows, :] = (gate * jax.nn.sigmoid(gate) * gu[:, C:]).astype(BF16)
            put(da, c, rows, dot(act[rows, :], wdc[...]))

        @pl.when(c < PIECES - 1)
        def _():
            down_copy(0, c + 1).start()

    start(up_copies(1, 0))
    down_copy(1, 0).start()
    wait(bring[1:])

    @pl.loop(0, T // 128)
    def _(i):
        rows = aligned(i, 128)
        h = dgu[rows, :D] + da[rows, :].astype(BF16)
        dgu[rows, :D] = h
        low = norm(h)
        a[rows, :] = low
        at[:, rows] = low.T
        dt[:, rows] = d[rows, :].T

    keep = local(wide_rows(dgu), h1, load_sem.at[0])
    keep.start()
    pl.semaphore_wait(barrier, 3)
    keep.wait()

    chunks(1)

    bring = local(h1, a, load_sem.at[0])
    bring.start()
    start(up_copies(1, 0))
    dgu_copy(PIECES - 1, every, False, load_sem.at[2]).wait()
    tiles = T // TILE

    @pl.loop(0, tiles)
    def _(i):
        dgu_copy(0, aligned(i, TILE), True, tile_sem.at[i]).start()

    @pl.loop(0, PIECES)
    def _(c):
        s = c + PIECES
        wait(up_copies(1, c))
        next_up(1, c)

        def tokens(i):
            rows = aligned(i, TILE)
            dgu_copy(c, rows, True, tile_sem.at[i]).wait()
            put(da, c, rows, dot(dgu[rows, :], wgu[lax.rem(c, 2)], 1, 1))

            @pl.when(c < PIECES - 1)
            def _():
                dgu_copy(c + 1, rows, True, tile_sem.at[i]).start()

        pl.loop(0, tiles // 2)(tokens)
        before(s)
        send(s)
        pl.loop(tiles // 2, tiles)(tokens)
        after(s)

    again = local(x, wide_rows(dgu), load_sem.at[1])
    again.start()
    start(up_copies(0, 0))
    down_copy(0, 0).start()
    bring.wait()

    @pl.loop(0, T // 128)
    def _(i):
        rows = aligned(i, 128)
        wide = a[rows, :].astype(F32)
        scale = lax.rsqrt(jnp.mean(wide * wide, -1, keepdims=True) + 1e-6)
        by = da[rows, :].astype(BF16).astype(F32)
        inner = jnp.mean(wide * by, -1, keepdims=True)
        total = d[rows, :] + (by * scale - wide * (inner * scale * scale * scale)).astype(BF16)
        d[rows, :] = total
        dt[:, rows] = total.T

    again.wait()

    @pl.loop(0, T // 128)
    def _(i):
        rows = aligned(i, 128)
        low = norm(dgu[rows, :D])
        a[rows, :] = low
        at[:, rows] = low.T

    chunks(0)

    @pl.loop(3 * PIECES, 4 * PIECES + 5)
    def _(s):
        before(s)
        send(s)
        after(s)


def gathered_step(mesh, dims, operands):
    T, D, FF, C, R, RB, PB = dims
    hbm = pl.BlockSpec(memory_space=pl.ANY)
    vmem, dma = pltpu.VMEM, pltpu.SemaphoreType.DMA
    shapes = [vmem((T, D), BF16), vmem((D, T), BF16), vmem((T, D), BF16), vmem((D, T), BF16), vmem((T, D), F32)]
    shapes += [vmem((2, D, 2 * C), BF16), vmem((C, D), BF16), vmem((T, C), BF16), vmem((T, 2 * C), BF16)]
    shapes += [vmem((8, PB, D), BF16), vmem((2, 2, 4, 2, R, C), BF16)]
    shapes += [dma((3,)), dma((2, 3)), dma, dma((T // TILE,))]
    for na, r, n, half in ((2, R, C, (2, R // 2, C)), (1, PB, D, (1, PB, D // 2))):
        tile = (na, r, n)
        shapes += [vmem((2, na, 4, r, n), BF16), vmem((2, *tile), BF16), vmem((2, 2, *half), BF16), vmem((2, 2, *tile), BF16),
                   vmem((2, 2, *tile), BF16), vmem(tile, F32), vmem(tile, F32), vmem(tile, BF16), vmem((2, *tile), BF16),
                   vmem((2, *tile), BF16)]
        shapes += [dma((2,)), dma((2,)), dma((2, 2)), dma((2, 2)), dma((2, 2)), dma((2, 2))]
        shapes += [dma((8, 2)), dma((8, 2)), dma((8, 2)), dma((8, 2)), dma((8, 4)), dma((8, 4)), dma((6,)), dma((2, 2)),
                   pltpu.SemaphoreType.REGULAR]
    shapes += [vmem((2, 1, 4, PB, D), BF16), dma((2,))]
    out = lambda *s: jax.ShapeDtypeStruct(s, BF16)
    L = 2
    return pl.pallas_call(
        functools.partial(kernel, dims),
        out_shape=(out(L, D, FF), out(L, D, FF), out(L, FF, D), out(L, 2, R, FF), out(L, RB, D), out(L, 8 * PIECES, PB, D),
                   out(T, D), out(PIECES, T, 2 * C)),
        in_specs=[hbm] * len(operands),
        out_specs=(hbm,) * 8,
        scratch_shapes=shapes,
        compiler_params=pltpu.CompilerParams(collective_id=0, has_side_effects=True, vmem_limit_bytes=67_000_000),
        name="step",
    )(*operands)


def solution(mesh):
    assert mesh.shape["dp"] == 8

    def body(x, dy, wg, wu, wd, mg, mu, md, vg, vu, vd):
        T, D = x.shape[1:]
        FF = wg.shape[2]
        dims = (T, D, FF, FF // PIECES, D // 8, FF // 8, FF // 8 // PIECES)
        nw_g, nw_u, nw_d, g_a, g_b, *_ = gathered_step(mesh, dims, (x[0], dy[0], wg, wu, wd, mg, mu, md, vg, vu, vd))
        g = [g_a[:, 0], g_a[:, 1], g_b]
        new = [new_moments(m, v, t.astype(F32)) for m, v, t in zip((mg, mu, md), (vg, vu, vd), g, strict=True)]
        return (nw_g, nw_u, nw_d, *(t[0] for t in new), *(t[1] for t in new))

    seq, rep, rows = P(("rep", "dp")), P(), P(None, "dp")
    return jax.shard_map(
        body, mesh=mesh, in_specs=(seq, seq, rep, rep, rep) + (rows,) * 6,
        out_specs=(P("rep"),) * 3 + (P("rep", "dp"),) * 6, check_vma=False)
```
